16 devices in a mesh: rep: 4 (over y, z, core), dp: 4 (over x).
Axes of the slice: x: 4, y: 2, z: 1, core: 2. Of those that a mesh axis runs over, the one named last changes fastest.
The devices are a block of a 4x4x8 slice.
Arguments:
- x: bfloat16 [16, 4096, 768], P(('rep', 'dp')), parts along dimension 0
- dy: bfloat16 [16, 4096, 768], P(('rep', 'dp')), parts along dimension 0
- w_gate: bfloat16 [2, 768, 1792], P(None, 'dp')
- w_up: bfloat16 [2, 768, 1792], P(None, 'dp')
- w_down: bfloat16 [2, 1792, 768], P(None, 'dp')
- m_w_gate: float32 [2, 768, 1792], P(None, 'dp')
- m_w_up: float32 [2, 768, 1792], P(None, 'dp')
- m_w_down: float32 [2, 1792, 768], P(None, 'dp')
- v_w_gate: float32 [2, 768, 1792], P(None, 'dp')
- v_w_up: float32 [2, 768, 1792], P(None, 'dp')
- v_w_down: float32 [2, 1792, 768], P(None, 'dp')
Outputs:
- output 1: bfloat16 [8, 768, 1792], P('rep', 'dp'), parts along dimension 0
- output 2: bfloat16 [8, 768, 1792], P('rep', 'dp'), parts along dimension 0
- output 3: bfloat16 [8, 1792, 768], P('rep', 'dp'), parts along dimension 0
- output 4: float32 [8, 768, 1792], P('rep', 'dp'), parts along dimension 0
- output 5: float32 [8, 768, 1792], P('rep', 'dp'), parts along dimension 0
- output 6: float32 [8, 1792, 768], P('rep', 'dp'), parts along dimension 0
- output 7: float32 [8, 768, 1792], P('rep', 'dp'), parts along dimension 0
- output 8: float32 [8, 768, 1792], P('rep', 'dp'), parts along dimension 0
- output 9: float32 [8, 1792, 768], P('rep', 'dp'), parts along dimension 0
There are 4 independent parts. The reference program is written for one: setup_inputs(seed, part) draws one part's arguments, and reference() takes and returns one part's arrays. A program takes and returns all parts, laid end to end along the dimension named above; an argument that names none is the same for every part.
All inputs are finite; a program needn't handle non-finite values.
Results may differ from the reference program's by a relative error of at most 0.022.
Values are sent between devices in bfloat16 or wider.
A program may use at most 768 MiB of HBM per device.

```python
import jax
import jax.numpy as jnp
from jax import lax

SEQUENCES = 4
TOKENS = 4096
D = 768
FF = 1792
LAYERS = 2
NAMES = ("w_gate", "w_up", "w_down")
SHAPES = {"w_gate": (LAYERS, D, FF), "w_up": (LAYERS, D, FF), "w_down": (LAYERS, FF, D)}


def bump(key, n, height):
    away = (jnp.arange(n, dtype=jnp.int32) - jax.random.randint(key, (), 0, n, jnp.int32)) % n
    return jnp.where(away < n // 8, height, 1.0)


def together(key, own, strength):
    shared = jax.random.normal(key, own.shape[1:], jnp.float32)
    return (own + strength * shared) * lax.rsqrt(1 + strength * strength)


def setup_inputs(seed: int = 0, part: int = 0) -> dict:
    kx, kdy, ka, kb, kz, kf, kh, kl, *keys = jax.random.split(jax.random.key(seed), 8 + 3 * len(NAMES))
    kx, kdy, ka, kb = (jax.random.fold_in(k, part) for k in (kx, kdy, ka, kb))
    kw, km, kv = (keys[i::3] for i in range(3))
    shape = (SEQUENCES, TOKENS, D)
    much_x, much_dy = jax.random.uniform(kz, (2,), jnp.float32, 0.0, 1.0)
    loud = 2.0 ** jax.random.uniform(jax.random.fold_in(kz, 1), (), jnp.float32, -1.0, 2.0)
    layers = 2.0 ** jax.random.uniform(kl, (LAYERS, 1, 1), jnp.float32, -1.0, 1.0)
    x = together(ka, jax.random.normal(kx, shape, jnp.float32), much_x) * bump(kf, D, 4.0)
    dy = together(kb, jax.random.normal(kdy, shape, jnp.float32), much_dy)
    drawn = {"x": x.astype(jnp.bfloat16), "dy": (loud * dy * (SEQUENCES * TOKENS) ** -0.5).astype(jnp.bfloat16)}
    for key, name in zip(kw, NAMES, strict=True):
        w = jax.random.normal(key, SHAPES[name], jnp.float32) * SHAPES[name][1] ** -0.5
        drawn[name] = (w * {"w_gate": 1.0, "w_up": bump(kh, FF, 4.0), "w_down": layers}[name]).astype(jnp.bfloat16)
    for key, name in zip(km, NAMES, strict=True):
        drawn[f"m_{name}"] = 0.1 * jax.random.normal(key, SHAPES[name], jnp.float32)
    for key, name in zip(kv, NAMES, strict=True):
        drawn[f"v_{name}"] = jax.random.uniform(key, SHAPES[name], jnp.float32, 0.005, 0.015)
    return drawn


def matmul(a, w):
    return jnp.dot(a, w, preferred_element_type=jnp.float32).astype(jnp.bfloat16)


def normed(h):
    wide = h.astype(jnp.float32)
    scale = lax.rsqrt(jnp.mean(wide**2, -1, keepdims=True) + 1e-6)
    return (wide * scale).astype(jnp.bfloat16)


def layer(h, w):
    a = normed(h)
    gate = jnp.dot(a, w["w_gate"], preferred_element_type=jnp.float32)
    up = jnp.dot(a, w["w_up"], preferred_element_type=jnp.float32)
    return h + matmul((jax.nn.silu(gate) * up).astype(jnp.bfloat16), w["w_down"])


def adamw(w, m, v, g):
    m = 0.9 * m + 0.1 * g
    v = 0.95 * v + 0.05 * g * g
    step = m * lax.rsqrt(v + 1e-8) + 0.1 * w
    return (w - 0.02 * step).astype(jnp.bfloat16), m, v


def clipped(gradients, sum_of_squares, count):
    factor = jnp.minimum(1.0, 0.5 * lax.rsqrt(sum_of_squares / count + 1e-30))
    return [g * factor for g in gradients]


def stack(weights, h):
    return lax.scan(lambda h, w: (layer(h, w), None), h, weights)[0]


def reference(x, dy, w_gate, w_up, w_down, m_w_gate, m_w_up, m_w_down, v_w_gate, v_w_up, v_w_down):
    weights = dict(zip(NAMES, (w_gate, w_up, w_down), strict=True))

    def take(so_far, sequence):
        h, by_y = sequence
        _, back = jax.vjp(lambda w: stack(w, h), weights)
        return jax.tree.map(lambda total, term: total + term.astype(jnp.float32), so_far, back(by_y)[0]), None

    none_yet = {name: jnp.zeros(w.shape, jnp.float32) for name, w in weights.items()}
    by_weights, _ = lax.scan(take, none_yet, (x, dy))
    gradients = [by_weights[name].astype(jnp.bfloat16).astype(jnp.float32) for name in NAMES]
    gradients = clipped(gradients, sum(jnp.sum(g * g) for g in gradients), sum(g.size for g in gradients))
    new = [
        adamw(w.astype(jnp.float32), m, v, g)
        for w, m, v, g in zip((w_gate, w_up, w_down), (m_w_gate, m_w_up, m_w_down), (v_w_gate, v_w_up, v_w_down), gradients, strict=True)
    ]
    return tuple(one[which] for which in range(3) for one in new)
```

```python
import functools

import jax
import jax.numpy as jnp
from jax import lax
from jax.experimental import pallas as pl
from jax.experimental.pallas import tpu as pltpu
from jax.sharding import PartitionSpec as P

MESH = pl.DeviceIdType.MESH
F32, BF16 = jnp.float32, jnp.bfloat16
ANY = pl.BlockSpec(memory_space=pl.ANY)
IN_VMEM = pl.BlockSpec(memory_space=pltpu.VMEM)
DMA = pltpu.SemaphoreType.DMA
MIB = 2**20
WIDTH = 64


def dot(a, b, ca=1, cb=0):
    return lax.dot_general(a, b, (((ca,), (cb,)), ((), ())), preferred_element_type=F32)


def rows(index, size):
    return pl.ds(pl.multiple_of(index * size, size), size)


def at(start, size):
    return pl.ds(pl.multiple_of(start, 16), size)


def normed(h):
    wide = h.astype(F32)
    scale = lax.rsqrt(jnp.mean(wide * wide, -1, keepdims=True) + 1e-6)
    return (wide * scale).astype(BF16)


def around(n):
    me = lax.axis_index("dp")
    return me, lax.rem(me + n - 1, n), lax.rem(me + 1, n), lax.rem(me + 2, n)


def meet(where):
    barrier = pltpu.get_barrier_semaphore()
    for device in where:
        pl.semaphore_signal(barrier, inc=1, device_id=device, device_id_type=MESH)
    pl.semaphore_wait(barrier, len(where))


def remote(source, target, send, receive, device):
    return pltpu.make_async_remote_copy(
        src_ref=source, dst_ref=target, send_sem=send, recv_sem=receive, device_id=device, device_id_type=MESH
    )


KINDS = 18


def forward_kernel(
    n, x_h, dy_h, wg, wu, wd, gu_o, d_o, a_o, at_o, dyt_o, h_o, a1_o, a1t_o,
    xv, av, dyv, acts, gw, dw, packed, tst, tst2, hst, ast, ssem, rsem, xsem, dysem, osem, wsem,
):
    layers, chunks = gw.shape[0], gw.shape[1]
    tokens, dim = xv.shape
    own, hidden = wg.shape[1], dw.shape[2]
    share, third = wd.shape[1] // chunks, own // 4
    steps = layers * chunks
    tile = dyv.shape[1]
    tiles = tokens // tile
    me, left, right, across = around(n)
    rep = lax.axis_index("rep")
    core, side = lax.rem(rep, 2), lax.rem(rep // 2, 2)
    mate, twin = rep + 1 - 2 * core, rep + 2 - 4 * side

    def x_in(t):
        return pltpu.make_async_copy(x_h.at[rows(t, tile)], xv.at[rows(t, tile)], xsem.at[t])

    def dy_in(t):
        return pltpu.make_async_copy(dy_h.at[rows(t, tile)], dyv.at[lax.rem(t, 2)], dysem.at[lax.rem(t, 2)])

    def start_x(t, _):
        x_in(t).start()
        return 0

    lax.fori_loop(0, tiles, start_x, 0)
    dy_in(0).start()
    dy_in(1).start()

    for layer in range(layers):
        gate, up = wg[layer], wu[layer]
        for j in range(chunks):
            pieces = [w[:, o * share * chunks + j * share : o * share * chunks + (j + 1) * share] for w in (gate, up) for o in range(n)]
            packed[layer * chunks + j] = jnp.concatenate(pieces, -1)

    def place(s, _):
        layer, j = s // chunks, lax.rem(s, chunks)
        gw[layer, j, at(me * own, own), :] = packed[s]
        dw[layer, j, at(me * share, share), :] = wd[layer, rows(j, share), :]
        return 0

    lax.fori_loop(0, steps, place, 0)

    meet([{"dp": left}, {"dp": right}, {"rep": mate}, {"rep": twin}])

    def up_part(s, owner, which):
        return gw.at[s // chunks, lax.rem(s, chunks), at(owner * own + which * 2 * third + core * third, third), :]

    def down_part(s, owner):
        return dw.at[s // chunks, lax.rem(s, chunks), at(owner * share + core * (share // 2), share // 2), :]

    others = (left, right, across)

    def copy(s, kind):
        if kind < 4:
            ref = down_part(s, me) if kind % 2 else up_part(s, me, side)
            device = {"dp": right if kind < 2 else left}
        elif kind == 4:
            ref, device = up_part(s, left, side), {"dp": right}
        elif kind == 5:
            ref, device = down_part(s, right), {"dp": left}
        elif kind < 9:
            ref, device = up_part(s, others[kind - 6], side), {"rep": twin}
        elif kind < 15:
            owner = others[(kind - 9) // 2]
            ref, device = (up_part(s, owner, side) if kind % 2 else down_part(s, owner)), {"rep": mate}
        else:
            ref, device = up_part(s, others[kind - 15], 1 - side), {"rep": mate}
        return remote(ref, ref, ssem.at[s, kind], rsem.at[s, kind], device)

    def weights_out(s):
        layer, j = s // chunks, lax.rem(s, chunks)
        return (
            pltpu.make_async_copy(gw.at[layer, j], gu_o.at[layer, j], wsem.at[s, 0]),
            pltpu.make_async_copy(dw.at[layer, j], d_o.at[layer, j], wsem.at[s, 1]),
        )

    def stage(s, wait, begin):
        @pl.when((s >= 0) & (s < steps))
        def _():
            for kind in wait:
                copy(s, kind).wait_recv()
            for kind in begin:
                copy(s, kind).start()

    def tick(k):
        stage(k + 1, (), (0, 1, 2, 3))
        stage(k - 1, (0, 1, 2, 3), (4, 5, 6, 7, 9, 10, 11, 12))
        stage(k - 2, (4, 5), (8, 13, 14))
        stage(k - 3, (6, 7, 8), (15, 16, 17))
        stage(k - 4, range(9, KINDS), ())

        @pl.when((k >= 4) & (k - 4 < steps))
        def _():
            for c in weights_out(k - 4):
                c.start()

    def at_out(t, slot):
        return pltpu.make_async_copy(tst.at[slot], at_o.at[:, rows(t, tile)], osem.at[slot, 0])

    def dyt_out(t, slot):
        return pltpu.make_async_copy(tst2.at[slot], dyt_o.at[:, rows(t, tile)], osem.at[slot, 1])

    def prepare(t, slot):
        x_in(t).wait()
        dy_in(t).wait()

        @pl.when(t >= 2)
        def _():
            at_out(t, slot).wait()
            dyt_out(t, slot).wait()

        a = normed(xv[rows(t, tile), :])
        av[rows(t, tile), :] = a
        tst[slot] = a.T
        tst2[slot] = dyv[slot].T
        at_out(t, slot).start()
        dyt_out(t, slot).start()

        @pl.when(t + 2 < tiles)
        def _():
            dy_in(t + 2).start()

    stage(0, (), (0, 1, 2, 3))

    def open_(k, _):
        tick(k)
        prepare(2 * k, 0)
        prepare(2 * k + 1, 1)
        return 0

    lax.fori_loop(0, 4, open_, 0)
    tick(4)
    a_out = pltpu.make_async_copy(av, a_o, osem.at[0, 2])
    a_out.start()
    big = 2 * tile

    def chunk(j, _):
        def part(t, _):
            gu = dot(av[rows(t, big), :], gw[0, j])
            gate, up = gu[:, :hidden], gu[:, hidden:]
            acts[rows(t, big), rows(j, hidden)] = (gate * jax.nn.sigmoid(gate) * up).astype(BF16)
            return 0

        lax.fori_loop(0, tokens // big, part, 0)
        tick(j + 5)
        return 0

    lax.fori_loop(0, chunks, chunk, 0)
    for slot in range(2):
        at_out(0, slot).wait()
        dyt_out(0, slot).wait()

    def outs(t):
        slot = lax.rem(t, 2)
        return (
            pltpu.make_async_copy(hst.at[slot], h_o.at[rows(t, tile)], osem.at[slot, 3]),
            pltpu.make_async_copy(ast.at[slot], a1_o.at[rows(t, tile)], osem.at[slot, 4]),
            pltpu.make_async_copy(tst.at[slot], a1t_o.at[:, rows(t, tile)], osem.at[slot, 5]),
        )

    def close(t, _):
        slot = lax.rem(t, 2)

        @pl.when(t >= 2)
        def _():
            for c in outs(t):
                c.wait()

        y = dot(acts[rows(t, tile), :], dw[0].reshape(chunks * hidden, dim)).astype(BF16)
        h = (xv[rows(t, tile), :].astype(F32) + y.astype(F32)).astype(BF16)
        a = normed(h)
        hst[slot] = h
        ast[slot] = a
        tst[slot] = a.T
        for c in outs(t):
            c.start()
        tick(chunks + 5 + t)
        return 0

    lax.fori_loop(0, tiles, close, 0)
    for t in (tiles - 2, tiles - 1):
        for c in outs(t):
            c.wait()
    a_out.wait()

    def finish(s, _):
        for kind in range(KINDS):
            copy(s, kind).wait_send()
        for c in weights_out(s):
            c.wait()
        return 0

    lax.fori_loop(0, steps, finish, 0)


def forward(n, x, dy, wg, wu, wd):
    tokens, dim = x.shape
    layers, own, units = wg.shape
    chunks = wd.shape[1] // WIDTH
    hidden = n * WIDTH
    tile = 512
    V = pltpu.VMEM
    S = jax.ShapeDtypeStruct
    return pl.pallas_call(
        functools.partial(forward_kernel, n),
        out_shape=[
            S((layers, chunks, dim, 2 * hidden), BF16), S((layers, chunks, hidden, dim), BF16),
            S((tokens, dim), BF16), S((dim, tokens), BF16), S((dim, tokens), BF16),
            S((tokens, dim), BF16), S((tokens, dim), BF16), S((dim, tokens), BF16),
        ],
        in_specs=[ANY, ANY, IN_VMEM, IN_VMEM, IN_VMEM],
        out_specs=[ANY] * 8,
        scratch_shapes=[
            V((tokens, dim), BF16), V((tokens, dim), BF16), V((2, tile, dim), BF16), V((tokens, units), BF16),
            V((layers, chunks, dim, 2 * hidden), BF16), V((layers, chunks, hidden, dim), BF16),
            V((layers * chunks, own, 2 * hidden), BF16), V((2, dim, tile), BF16), V((2, dim, tile), BF16), V((2, tile, dim), BF16), V((2, tile, dim), BF16),
            DMA((layers * chunks, KINDS)), DMA((layers * chunks, KINDS)),
            DMA((tokens // tile,)), DMA((2,)), DMA((2, 6)), DMA((layers * chunks, 2)),
        ],
        compiler_params=pltpu.CompilerParams(collective_id=0, has_side_effects=True, vmem_limit_bytes=63 * MIB),
        name="forward",
    )(x, dy, wg, wu, wd)


def backward_kernel(n, deep, *refs):
    it = iter(refs)
    take = lambda count: [next(it) for _ in range(count)]
    a_h, at_h, dy_h, dyt_h, gu_all, d_all, extra = take(7)
    gu_h, d_h = gu_all.at[1 if deep else 0], d_all.at[1 if deep else 0]
    og, od, sq = take(3)
    if deep:
        dgu_o, dx_o, dxt_o = take(3)
    av, atv, dyv, dytv, dgu, act, gw, dw, tg, td, rg, rd, sqg, sqd, ssem, rsem, isem, wsem = take(18)
    if deep:
        flat, wide, hst, xtst, dsem, fsem, psem, osem = take(8)
    else:
        tot, csem = take(2)
    tokens, dim = av.shape
    chunks, hidden = d_all.shape[1:3]
    own, share = dim // n, hidden // n
    g2, d2 = own // 2, share // 2
    big = 1024
    parts = tokens // big
    me, left, right, across = around(n)

    def a_in(t):
        return pltpu.make_async_copy(a_h.at[rows(t, big)], av.at[rows(t, big)], isem.at[0, t])

    def dy_in(t):
        return pltpu.make_async_copy(dy_h.at[rows(t, big)], dyv.at[rows(t, big)], isem.at[1, t])

    late = (pltpu.make_async_copy(at_h, atv, isem.at[2, 0]), pltpu.make_async_copy(dyt_h, dytv, isem.at[2, 1]))

    def w_in(j):
        s = lax.rem(j, 2)
        return (pltpu.make_async_copy(gu_h.at[j], gw.at[s], wsem.at[s, 0]), pltpu.make_async_copy(d_h.at[j], dw.at[s], wsem.at[s, 1]))

    for c in w_in(0):
        c.start()
    for t in range(parts):
        a_in(t).start()
        dy_in(t).start()
    for c in late:
        c.start()
    sqg[...] = jnp.zeros_like(sqg)
    sqd[...] = jnp.zeros_like(sqd)
    meet([{"dp": left}, {"dp": right}] + ([] if deep else [{"dp": across}]))

    def copy(j, unit, matrix):
        slot = lax.rem(j, 3)
        term, half, block = (tg, g2, own) if matrix == 0 else (td, d2, share)
        device = {"dp": right if unit % 2 == 0 else left}
        if unit < 2:
            source = term.at[slot, at(across * block + unit * half, half), :]
        elif unit < 4:
            owner, which = (right, 1) if unit == 2 else (left, 0)
            source = term.at[slot, at(owner * block + which * half, half), :]
        else:
            owner, which = (right, 0) if unit == 4 else (left, 1)
            source = term.at[slot, at(owner * block + which * half, half), :]
        target = (rg if matrix == 0 else rd).at[j, unit]
        return remote(source, target, ssem.at[j, 2 * unit + matrix], rsem.at[j, 2 * unit + matrix], device)

    def send_terms(j):
        for unit in (0, 1, 2, 3):
            for matrix in (0, 1):
                copy(j, unit, matrix).start()

    def pass_on(j):
        slot = lax.rem(j, 3)
        for unit in (0, 1):
            owner = right if unit == 0 else left
            for matrix, (term, half, block, got) in enumerate(((tg, g2, own, rg), (td, d2, share, rd))):
                copy(j, unit, matrix).wait_recv()
                place = at(owner * block + unit * half, half)
                term[slot, place, :] = (term[slot, place, :].astype(F32) + got[j, unit].astype(F32)).astype(BF16)
                copy(j, unit + 4, matrix).start()

    def settle(j):
        slot = lax.rem(j, 3)
        for unit in (2, 3, 4, 5):
            for matrix in (0, 1):
                copy(j, unit, matrix).wait_recv()
        for matrix, (term, half, block, got, out, total) in enumerate(((tg, g2, own, rg, og, sqg), (td, d2, share, rd, od, sqd))):
            for which in (0, 1):
                mine = term[slot, at(me * block + which * half, half), :].astype(F32)
                single, summed = (3, 4) if which == 0 else (2, 5)
                g = (mine + got[j, single].astype(F32) + got[j, summed].astype(F32)).astype(BF16)
                out[j, which * half : (which + 1) * half, :] = g
                g = g.astype(F32)
                total[...] += jnp.sum((g * g).reshape(half // 8, 8, g.shape[-1]), axis=0)
        for unit in range(6):
            for matrix in (0, 1):
                copy(j, unit, matrix).wait_send()

    if deep:
        dgu_out = lambda j: pltpu.make_async_copy(dgu, dgu_o.at[:, rows(j, 2 * hidden)], dsem.at[0])
        flat_in = lambda j: pltpu.make_async_copy(gu_h.at[j], flat.at[:, j * 2 * hidden : (j + 1) * 2 * hidden], fsem.at[j])

    def chunk(j, _):
        s, slot = lax.rem(j, 2), lax.rem(j, 3)
        for c in w_in(j):
            c.wait()

        @pl.when(j + 1 < chunks)
        def _():
            for c in w_in(j + 1):
                c.start()

        if deep:

            @pl.when(j >= 1)
            def _():
                dgu_out(j - 1).wait()

        def part(t, _):
            @pl.when(j == 0)
            def _():
                a_in(t).wait()
                dy_in(t).wait()

            r = rows(t, big)
            gu = dot(av[r, :], gw[s])
            dact = dot(dyv[r, :], dw[s], 1, 1).astype(BF16).astype(F32)
            gate, up = gu[:, :hidden], gu[:, hidden:]
            sig = jax.nn.sigmoid(gate)
            silu = gate * sig
            act[r, :] = (silu * up).astype(BF16)
            dgu[r, hidden:] = (dact * silu).astype(BF16)
            dgu[r, :hidden] = (dact * up * (sig + silu * (1 - sig))).astype(BF16)
            return 0

        lax.fori_loop(0, parts, part, 0)
        if deep:
            dgu_out(j).start()

        @pl.when(j == 0)
        def _():
            for c in late:
                c.wait()

        tg[slot] = dot(atv[...], dgu[...]).astype(BF16)
        td[slot] = dot(dytv[...], act[...]).T.astype(BF16)

        @pl.when(j >= 1)
        def _():
            pass_on(j - 1)

        send_terms(j)

        @pl.when(j >= 2)
        def _():
            settle(j - 2)

        return 0

    if deep:
        for j in range(chunks):
            flat_in(j).start()
    lax.fori_loop(0, chunks, chunk, 0)
    last = chunks - 1
    if deep:
        for j in range(chunks):
            flat_in(j).wait()
        dgu_out(last).wait()
        tile = wide.shape[1]
        tiles = tokens // tile

        def ins(t):
            s = lax.rem(t, 2)
            return (
                pltpu.make_async_copy(dgu_o.at[rows(t, tile)], wide.at[s], psem.at[s, 0]),
                pltpu.make_async_copy(extra.at[rows(t, tile)], hst.at[s], psem.at[s, 1]),
            )

        def outs(t):
            s = lax.rem(t, 2)
            return (
                pltpu.make_async_copy(dyv.at[rows(t, tile)], dx_o.at[rows(t, tile)], osem.at[s, 0]),
                pltpu.make_async_copy(xtst.at[s], dxt_o.at[:, rows(t, tile)], osem.at[s, 1]),
            )

        for c in ins(0):
            c.start()

        def part(t, _):
            s = lax.rem(t, 2)
            for c in ins(t):
                c.wait()

            @pl.when(t + 1 < tiles)
            def _():
                for c in ins(t + 1):
                    c.start()

            @pl.when(t >= 2)
            def _():
                for c in outs(t):
                    c.wait()

            da = dot(wide[s], flat[...], 1, 1).astype(BF16).astype(F32)
            h = hst[s].astype(F32)
            scale = lax.rsqrt(jnp.mean(h * h, -1, keepdims=True) + 1e-6)
            along = jnp.sum(da * h, -1, keepdims=True) * (scale * scale * scale * (1.0 / dim))
            dh = (da * scale - h * along).astype(BF16)
            dx = (dyv[rows(t, tile), :].astype(F32) + dh.astype(F32)).astype(BF16)
            dyv[rows(t, tile), :] = dx
            xtst[s] = dx.T
            for c in outs(t):
                c.start()

            @pl.when(t == tiles // 4)
            def _():
                settle(last - 1)

            @pl.when(t == tiles // 2)
            def _():
                pass_on(last)

            return 0

        lax.fori_loop(0, tiles, part, 0)
        for t in (tiles - 2, tiles - 1):
            for c in outs(t):
                c.wait()
    else:
        settle(last - 1)
        pass_on(last)
    settle(last)

    total = sum(sqg[:, i * 128 : (i + 1) * 128] for i in range(sqg.shape[1] // 128))
    total += sum(sqd[:, i * 128 : (i + 1) * 128] for i in range(sqd.shape[1] // 128))
    if deep:
        sq[...] = total
    else:
        tot[me] = total + extra[...]
        peers = (left, right, across)

        def share_out(k):
            return remote(tot.at[me], tot.at[me], csem.at[0, k], csem.at[1, k], {"dp": peers[k]})

        for k in range(3):
            share_out(k).start()
    if not deep:
        for k in range(3):
            share_out(k).wait_send()
            share_out(k).wait_recv()
        sq[...] = tot[0] + tot[1] + tot[2] + tot[3]


def backward(n, deep, a, at_, dy, dyt, gu, d, extra):
    tokens, dim = a.shape
    chunks, hidden = d.shape[1:3]
    own, share = dim // n, hidden // n
    V = pltpu.VMEM
    S = jax.ShapeDtypeStruct
    tile = 256
    out_shape = [S((chunks, own, 2 * hidden), BF16), S((chunks, share, dim), BF16), S((8, 128), F32)]
    out_specs = [IN_VMEM] * 3
    scratch = [
        V((tokens, dim), BF16), V((dim, tokens), BF16), V((tokens, dim), BF16), V((dim, tokens), BF16),
        V((tokens, 2 * hidden), BF16), V((tokens, hidden), BF16), V((2, dim, 2 * hidden), BF16), V((2, hidden, dim), BF16),
        V((3, dim, 2 * hidden), BF16), V((3, hidden, dim), BF16),
        V((chunks, 6, own // 2, 2 * hidden), BF16), V((chunks, 6, share // 2, dim), BF16),
        V((8, 2 * hidden), F32), V((8, dim), F32),
        DMA((chunks, 12)), DMA((chunks, 12)), DMA((3, tokens // 1024)), DMA((2, 2)),
    ]
    if deep:
        out_shape += [S((tokens, chunks * 2 * hidden), BF16), S((tokens, dim), BF16), S((dim, tokens), BF16)]
        out_specs += [ANY] * 3
        scratch += [
            V((dim, chunks * 2 * hidden), BF16), V((2, tile, chunks * 2 * hidden), BF16), V((2, tile, dim), BF16),
            V((2, dim, tile), BF16), DMA((1,)), DMA((chunks,)), DMA((2, 2)), DMA((2, 2)),
        ]
    else:
        scratch += [V((n, 8, 128), F32), DMA((2, 3))]
    return pl.pallas_call(
        functools.partial(backward_kernel, n, deep),
        out_shape=out_shape,
        in_specs=[ANY] * 6 + [ANY if deep else IN_VMEM],
        out_specs=out_specs,
        scratch_shapes=scratch,
        compiler_params=pltpu.CompilerParams(collective_id=1 if deep else 2, has_side_effects=True, vmem_limit_bytes=63 * MIB),
        name="backward_deep" if deep else "backward_first",
    )(a, at_, dy, dyt, gu, d, extra)


def update_kernel(n, count, sq, g0, g1, d0, d1, wg, wu, wd, mg, mu, md, vg, vu, vd, *outs):
    factor = jnp.minimum(1.0, 0.5 * lax.rsqrt(jnp.sum(sq[...], keepdims=True) / count + 1e-30))
    first = pl.program_id(0) == 0
    gu = jnp.where(first, g0[...], g1[...]).astype(F32)
    chunks, hidden = gu.shape[0], gu.shape[2] // 2
    share = hidden // n

    def ordered(start):
        return jnp.concatenate([gu[j, :, start + o * share : start + (o + 1) * share] for o in range(n) for j in range(chunks)], -1)

    grads = (ordered(0), ordered(hidden), jnp.where(first, d0[...], d1[...]).astype(F32))
    for i, (g, w, m, v) in enumerate(zip(grads, (wg, wu, wd), (mg, mu, md), (vg, vu, vd), strict=True)):
        g = g * factor
        new_m = 0.9 * m[0] + 0.1 * g
        new_v = 0.95 * v[0] + 0.05 * g * g
        step = new_m * lax.rsqrt(new_v + 1e-8) + 0.1 * w[0].astype(F32)
        outs[i][0] = (w[0].astype(F32) - 0.02 * step).astype(BF16)
        outs[3 + i][0] = new_m
        outs[6 + i][0] = new_v


def update(n, sq, g0, g1, d0, d1, weights, m, v):
    layers, own, units = weights[0].shape
    down, dim = weights[2].shape[1:]
    chunks = g0.shape[0]
    cut = 4
    count = float(n * sum(w.size for w in weights))
    up = pl.BlockSpec((1, own // cut, units), lambda i, k: (i, k, 0))
    dn = pl.BlockSpec((1, down // cut, dim), lambda i, k: (i, k, 0))
    gs = lambda which: pl.BlockSpec((chunks, own // cut, g0.shape[2]), lambda i, k: (0, jnp.where(i == which, k, (cut - 1) * (1 - which)), 0))
    ds = lambda which: pl.BlockSpec((down // cut, dim), lambda i, k: (jnp.where(i == which, k, (cut - 1) * (1 - which)), 0))
    three = [up, up, dn]
    return pl.pallas_call(
        functools.partial(update_kernel, n, count),
        grid=(layers, cut),
        out_shape=[jax.ShapeDtypeStruct(w.shape, t) for t in (BF16, F32, F32) for w in weights],
        in_specs=[pl.BlockSpec((8, 128), lambda i, k: (0, 0)), gs(0), gs(1), ds(0), ds(1)] + three * 3,
        out_specs=three * 3,
        compiler_params=pltpu.CompilerParams(vmem_limit_bytes=60 * MIB),
        name="update",
    )(sq, g0, g1, d0.reshape(down, dim), d1.reshape(down, dim), *weights, *m, *v)


def solution(mesh):
    n = mesh.shape["dp"]

    def step(x, dy, *arrays):
        weights, m, v = (arrays[i : i + 3] for i in (0, 3, 6))
        gu, d, a0, a0t, dyt, h1, a1, a1t = forward(n, x[0], dy[0], *weights)
        g1, d1, sq1, _, dx, dxt = backward(n, True, a1, a1t, dy[0], dyt, gu, d, h1)
        g0, d0, sq = backward(n, False, a0, a0t, dx, dxt, gu, d, sq1)
        return tuple(update(n, sq, g0, g1, d0, d1, weights, m, v))

    states, cut = P(("rep", "dp"), None, None), P(None, "dp", None)
    return jax.shard_map(
        step,
        mesh=mesh,
        in_specs=(states, states) + (cut,) * 9,
        out_specs=(P("rep", "dp", None),) * 9,
        check_vma=False,
    )
```

```python
import functools

import jax
import jax.numpy as jnp
from jax import lax
from jax.experimental import pallas as pl
from jax.experimental.pallas import tpu as pltpu
from jax.sharding import PartitionSpec as P

MESH = pl.DeviceIdType.MESH
F32, BF16 = jnp.float32, jnp.bfloat16
ANY = pl.BlockSpec(memory_space=pl.ANY)
IN_VMEM = pl.BlockSpec(memory_space=pltpu.VMEM)
DMA = pltpu.SemaphoreType.DMA
MIB = 2**20
WIDTH = 64


def dot(a, b, ca=1, cb=0):
    return lax.dot_general(a, b, (((ca,), (cb,)), ((), ())), preferred_element_type=F32)


def rows(index, size):
    return pl.ds(pl.multiple_of(index * size, size), size)


def at(start, size):
    return pl.ds(pl.multiple_of(start, 16), size)


def normed(h):
    wide = h.astype(F32)
    scale = lax.rsqrt(jnp.mean(wide * wide, -1, keepdims=True) + 1e-6)
    return (wide * scale).astype(BF16)


def around(n):
    me = lax.axis_index("dp")
    return me, lax.rem(me + n - 1, n), lax.rem(me + 1, n), lax.rem(me + 2, n)


def greet(where):
    for device in where:
        pl.semaphore_signal(pltpu.get_barrier_semaphore(), inc=1, device_id=device, device_id_type=MESH)


def meet(where):
    pl.semaphore_wait(pltpu.get_barrier_semaphore(), len(where))


def remote(source, target, send, receive, device):
    return pltpu.make_async_remote_copy(
        src_ref=source, dst_ref=target, send_sem=send, recv_sem=receive, device_id=device, device_id_type=MESH
    )


KINDS = 18


def forward_kernel(
    n, x_h, dy_h, wg, wu, wd, gu_o, d_o, kept_o, at_o, dyt_o, h_o, a1_o, a1t_o,
    xv, av, dyv, acts, gw, dw, gst, tst, tst2, hst, ast, ssem, rsem, xsem, dysem, osem, wsem, ksem,
):
    layers, chunks = gw.shape[0], gw.shape[1]
    tokens, dim = xv.shape
    own, hidden = wg.shape[1], dw.shape[2]
    share, piece = wd.shape[1] // chunks, own // 4
    steps = layers * chunks
    tile = dyv.shape[1]
    tiles = tokens // tile
    me, left, right, across = around(n)
    rep = lax.axis_index("rep")
    core, side = lax.rem(rep, 2), lax.rem(rep // 2, 2)
    mate, twin = rep + 1 - 2 * core, rep + 2 - 4 * side

    friends = [{"dp": left}, {"dp": right}, {"rep": mate}, {"rep": twin}]
    greet(friends)

    def x_in(t):
        return pltpu.make_async_copy(x_h.at[rows(t, tile)], xv.at[rows(t, tile)], xsem.at[t])

    def dy_in(t):
        return pltpu.make_async_copy(dy_h.at[rows(t, tile)], dyv.at[lax.rem(t, 2)], dysem.at[lax.rem(t, 2)])

    def start_x(t, _):
        x_in(t).start()
        return 0

    lax.fori_loop(0, tiles, start_x, 0)
    dy_in(0).start()
    dy_in(1).start()

    def pack(layer):
        gate, up = wg[layer], wu[layer]
        for j in range(chunks):
            pieces = [w[:, o * share * chunks + j * share : o * share * chunks + (j + 1) * share] for w in (gate, up) for o in range(n)]
            start = (layer * chunks + j) * own
            acts[start : start + own, : 2 * hidden] = jnp.concatenate(pieces, -1)

    def place(s, _):
        layer, j = s // chunks, lax.rem(s, chunks)
        gw[layer, j, at(me * own, own), :] = acts[rows(s, own), : 2 * hidden]
        dw[layer, j, at(me * share, share), :] = wd[layer, rows(j, share), :]
        return 0

    pack(0)
    lax.fori_loop(0, chunks, place, 0)
    meet(friends)

    def up_part(s, owner, which):
        return gw.at[s // chunks, lax.rem(s, chunks), at(owner * own + which * 2 * piece + core * piece, piece), :]

    def down_part(s, owner):
        return dw.at[s // chunks, lax.rem(s, chunks), at(owner * share + core * (share // 2), share // 2), :]

    others = (left, right, across)

    def copy(s, kind):
        if kind < 4:
            ref = down_part(s, me) if kind % 2 else up_part(s, me, side)
            device = {"dp": right if kind < 2 else left}
        elif kind == 4:
            ref, device = up_part(s, left, side), {"dp": right}
        elif kind == 5:
            ref, device = down_part(s, right), {"dp": left}
        elif kind < 9:
            ref, device = up_part(s, others[kind - 6], side), {"rep": twin}
        elif kind < 15:
            owner = others[(kind - 9) // 2]
            ref, device = (up_part(s, owner, side) if kind % 2 else down_part(s, owner)), {"rep": mate}
        else:
            ref, device = up_part(s, others[kind - 15], 1 - side), {"rep": mate}
        return remote(ref, ref, ssem.at[s, kind], rsem.at[s, kind], device)

    def weights_out(s):
        layer, j = s // chunks, lax.rem(s, chunks)
        return (
            pltpu.make_async_copy(gw.at[layer, j], gu_o.at[layer, j], wsem.at[s, 0]),
            pltpu.make_async_copy(dw.at[layer, j], d_o.at[layer, j], wsem.at[s, 1]),
        )

    def stage(s, wait, begin):
        @pl.when(s < steps)
        def _():
            for kind in wait:
                copy(s, kind).wait_recv()
            for kind in begin:
                copy(s, kind).start()

    first = ((), (0, 1, 2, 3))
    second = ((0, 1, 2, 3), (4, 5, 6, 7, 9, 10, 11, 12))
    third = ((4, 5), (8, 13, 14))
    fourth = ((6, 7, 8), (15, 16, 17))

    def arrived(s):
        stage(s, range(9, KINDS), ())

        @pl.when(s < steps)
        def _():
            for c in weights_out(s):
                c.start()

    def half_way(j):
        stage(j + 1, *fourth)
        stage(j + 4, *second)
        stage(j + 6, *first)

    def at_end(j):
        stage(j + 3, *third)
        arrived(j + 1)

    def at_out(t, slot):
        return pltpu.make_async_copy(tst.at[slot], at_o.at[:, rows(t, tile)], osem.at[slot, 0])

    def dyt_out(t, slot):
        return pltpu.make_async_copy(tst2.at[slot], dyt_o.at[:, rows(t, tile)], osem.at[slot, 1])

    def prepare(t, slot):
        x_in(t).wait()
        dy_in(t).wait()

        if t >= 2:
            at_out(t, slot).wait()
            dyt_out(t, slot).wait()

        a = normed(xv[rows(t, tile), :])
        av[rows(t, tile), :] = a
        tst[slot] = a.T
        tst2[slot] = dyv[slot].T
        at_out(t, slot).start()
        dyt_out(t, slot).start()

        if t + 2 < tiles:
            dy_in(t + 2).start()

    stage(0, *first)
    stage(1, *first)
    pack(1)
    lax.fori_loop(chunks, steps, place, 0)
    prepare(0, 0)
    prepare(1, 1)
    order = ((0, second), (2, first), 2, (1, second), (3, first), 3, (0, third), 4, (2, second), (4, first), 5, (1, third), 6, (0, fourth), 7)
    for item in order + ((3, second), (5, first), (2, third)):
        if isinstance(item, int):
            prepare(item, item % 2)
        else:
            stage(item[0], *item[1])
    arrived(0)
    big = 2 * tile
    parts = tokens // big

    def keep(j, t):
        return pltpu.make_async_copy(gst.at[lax.rem(t, 2)], kept_o.at[j, rows(t, big)], ksem.at[lax.rem(t, 2)])

    def chunk(j, _):
        def part(t, _):
            @pl.when((j > 0) | (t >= 2))
            def _():
                keep(j, t).wait()

            slot = lax.rem(t, 2)
            gu = dot(av[rows(t, big), :], gw[0, j])
            gst[slot] = gu
            keep(j, t).start()
            gate, up = gu[:, :hidden], gu[:, hidden:]
            acts[rows(t, big), rows(j, hidden)] = (gate * jax.nn.sigmoid(gate) * up).astype(BF16)
            return 0

        lax.fori_loop(0, parts // 2, part, 0)
        half_way(j)
        lax.fori_loop(parts // 2, parts, part, 0)
        at_end(j)
        return 0

    lax.fori_loop(0, chunks, chunk, 0)
    for slot in range(2):
        at_out(0, slot).wait()
        dyt_out(0, slot).wait()
        keep(chunks - 1, slot).wait()

    def outs(t):
        slot = lax.rem(t, 2)
        return (
            pltpu.make_async_copy(hst.at[slot], h_o.at[rows(t, tile)], osem.at[slot, 3]),
            pltpu.make_async_copy(ast.at[slot], a1_o.at[rows(t, tile)], osem.at[slot, 4]),
            pltpu.make_async_copy(tst.at[slot], a1t_o.at[:, rows(t, tile)], osem.at[slot, 5]),
        )

    def close(t, _):
        slot = lax.rem(t, 2)

        half_way(chunks + t)

        @pl.when(t >= 2)
        def _():
            for c in outs(t):
                c.wait()

        y = dot(acts[rows(t, tile), :], dw[0].reshape(chunks * hidden, dim)).astype(BF16)
        h = (xv[rows(t, tile), :].astype(F32) + y.astype(F32)).astype(BF16)
        a = normed(h)
        hst[slot] = h
        ast[slot] = a
        tst[slot] = a.T
        for c in outs(t):
            c.start()
        at_end(chunks + t)
        return 0

    lax.fori_loop(0, tiles, close, 0)
    for t in (tiles - 2, tiles - 1):
        for c in outs(t):
            c.wait()

    def finish(s, _):
        for kind in range(KINDS):
            copy(s, kind).wait_send()
        for c in weights_out(s):
            c.wait()
        return 0

    lax.fori_loop(0, steps, finish, 0)


def forward(n, x, dy, wg, wu, wd):
    tokens, dim = x.shape
    layers, own, units = wg.shape
    chunks = wd.shape[1] // WIDTH
    hidden = n * WIDTH
    tile = 512
    V = pltpu.VMEM
    S = jax.ShapeDtypeStruct
    return pl.pallas_call(
        functools.partial(forward_kernel, n),
        out_shape=[
            S((layers, chunks, dim, 2 * hidden), BF16), S((layers, chunks, hidden, dim), BF16),
            S((chunks, tokens, 2 * hidden), F32), S((dim, tokens), BF16), S((dim, tokens), BF16),
            S((tokens, dim), BF16), S((tokens, dim), BF16), S((dim, tokens), BF16),
        ],
        in_specs=[ANY, ANY, IN_VMEM, IN_VMEM, IN_VMEM],
        out_specs=[ANY] * 8,
        scratch_shapes=[
            V((tokens, dim), BF16), V((tokens, dim), BF16), V((2, tile, dim), BF16), V((tokens, units), BF16),
            V((layers, chunks, dim, 2 * hidden), BF16), V((layers, chunks, hidden, dim), BF16),
            V((2, 2 * tile, 2 * hidden), F32), V((2, dim, tile), BF16), V((2, dim, tile), BF16), V((2, tile, dim), BF16), V((2, tile, dim), BF16),
            DMA((layers * chunks, KINDS)), DMA((layers * chunks, KINDS)),
            DMA((tokens // tile,)), DMA((2,)), DMA((2, 6)), DMA((layers * chunks, 2)), DMA((2,)),
        ],
        compiler_params=pltpu.CompilerParams(collective_id=0, has_side_effects=True, vmem_limit_bytes=63 * MIB),
        name="forward",
    )(x, dy, wg, wu, wd)


def backward_kernel(n, deep, *refs):
    it = iter(refs)
    take = lambda count: [next(it) for _ in range(count)]
    a_h, at_h, dy_h, dyt_h, d_all, extra = take(6)
    d_h = d_all.at[1 if deep else 0]
    if deep:
        gu_h = next(it).at[1]
    og, od, sq = take(3)
    if deep:
        dgu_o, dx_o, dxt_o = take(3)
    av, atv, dyv, dytv, dgu, act, dw, tg, td, rg, rd, sqg, sqd, ssem, rsem, isem, wsem = take(17)
    if deep:
        gw, flat, wide, hst, xtst, dsem, fsem, psem, osem = take(9)
    else:
        tot, csem = take(2)
    tokens, dim = dyv.shape
    chunks, hidden = d_all.shape[1:3]
    own, share = dim // n, hidden // n
    g2, d2 = own // 2, share // 2
    big = 1024
    parts = tokens // big
    me, left, right, across = around(n)

    def a_in(t):
        return pltpu.make_async_copy(a_h.at[rows(t, big)], av.at[rows(t, big)], isem.at[0, t])

    def kept_in(j, t):
        return pltpu.make_async_copy(a_h.at[j, rows(t, big)], av.at[t], isem.at[0, t])

    def dy_in(t):
        return pltpu.make_async_copy(dy_h.at[rows(t, big)], dyv.at[rows(t, big)], isem.at[1, t])

    late = (pltpu.make_async_copy(dyt_h, dytv, isem.at[2, 0]), pltpu.make_async_copy(at_h, atv, isem.at[2, 1]))

    def w_in(j):
        s = lax.rem(j, 2)
        copies = [pltpu.make_async_copy(d_h.at[j], dw.at[s], wsem.at[s, 1])]
        if deep:
            copies.append(pltpu.make_async_copy(gu_h.at[j], gw.at[s], wsem.at[s, 0]))
        return copies

    friends = [{"dp": left}, {"dp": right}] + ([] if deep else [{"dp": across}])
    greet(friends)
    for c in w_in(0):
        c.start()
    if not deep:
        for t in range(parts):
            kept_in(0, t).start()
    for t in range(2):
        dy_in(t).start()
        if deep:
            a_in(t).start()
    sqg[...] = jnp.zeros_like(sqg)
    sqd[...] = jnp.zeros_like(sqd)
    meet(friends)

    def spot(j, matrix, owner, which):
        if matrix < 2:
            return tg, (lax.rem(j, 3), matrix, at(owner * own + which * g2, g2))
        return td, (lax.rem(j, 3), at(owner * share + which * d2, d2))

    def landing(j, unit, matrix):
        return (rg, (j, unit, matrix)) if matrix < 2 else (rd, (j, unit))

    def copy(j, unit, matrix):
        owner, which = ((across, 0), (across, 1), (right, 1), (left, 0), (right, 0), (left, 1))[unit]
        source, place = spot(j, matrix, owner, which)
        target, index = landing(j, unit, matrix)
        sem = 3 * unit + matrix
        return remote(source.at[place], target.at[index], ssem.at[j, sem], rsem.at[j, sem], {"dp": right if unit % 2 == 0 else left})

    def send_terms(j, matrix):
        for unit in (0, 1, 2, 3):
            copy(j, unit, matrix).start()

    def pass_on(j, matrix):
        for unit, owner, which in ((0, right, 0), (1, left, 1)):
            copy(j, unit, matrix).wait_recv()
            term, place = spot(j, matrix, owner, which)
            got, index = landing(j, unit, matrix)
            term[place] = (term[place].astype(F32) + got[index].astype(F32)).astype(BF16)
            copy(j, unit + 4, matrix).start()

    def settle(j, matrix):
        for unit in (2, 3, 4, 5):
            copy(j, unit, matrix).wait_recv()
        for which, single, summed in ((0, 3, 4), (1, 2, 5)):
            term, place = spot(j, matrix, me, which)
            got, one = landing(j, single, matrix)
            _, other = landing(j, summed, matrix)
            g = (term[place].astype(F32) + got[one].astype(F32) + got[other].astype(F32)).astype(BF16)
            if matrix < 2:
                og[j, which * g2 : (which + 1) * g2, matrix * hidden : (matrix + 1) * hidden] = g
            else:
                od[j, which * d2 : (which + 1) * d2, :] = g
            g = g.astype(F32)
            total = sqg if matrix < 2 else sqd
            total[...] += jnp.sum((g * g).reshape(g.shape[0] // 8, 8, g.shape[1]), axis=0)
        for unit in range(6):
            copy(j, unit, matrix).wait_send()

    def when(condition, what, *args):
        @pl.when(condition)
        def _():
            what(*args)

    if deep:
        dgu_out = lambda j: pltpu.make_async_copy(dgu, dgu_o.at[:, rows(j, 2 * hidden)], dsem.at[0])
        flat_in = lambda j: pltpu.make_async_copy(gu_h.at[j], flat.at[:, j * 2 * hidden : (j + 1) * 2 * hidden], fsem.at[j])

    def chunk(j, _):
        s, slot = lax.rem(j, 2), lax.rem(j, 3)
        for c in w_in(j):
            c.wait()

        @pl.when(j + 1 < chunks)
        def _():
            for c in w_in(j + 1):
                c.start()

        if deep:

            @pl.when(j >= 1)
            def _():
                dgu_out(j - 1).wait()

        def part(t, _):
            @pl.when(j == 0)
            def _():
                dy_in(t).wait()
                if deep:
                    a_in(t).wait()

                @pl.when(t + 2 < parts)
                def _():
                    dy_in(t + 2).start()
                    if deep:
                        a_in(t + 2).start()

                for i in range(2):
                    when(t == parts - 2 + i, late[i].start)

            r = rows(t, big)
            if deep:
                gu = dot(av[r, :], gw[s])
            else:
                kept_in(j, t).wait()
                gu = av[t]
            dact = dot(dyv[r, :], dw[s], 1, 1).astype(BF16).astype(F32)
            gate, up = gu[:, :hidden], gu[:, hidden:]
            sig = jax.nn.sigmoid(gate)
            silu = gate * sig
            act[r, :] = (silu * up).astype(BF16)
            dgu[r, hidden:] = (dact * silu).astype(BF16)
            dgu[r, :hidden] = (dact * up * (sig + silu * (1 - sig))).astype(BF16)
            if not deep:
                when(j + 1 < chunks, lambda: kept_in(j + 1, t).start())
            return 0

        lax.fori_loop(0, parts, part, 0)
        if deep:
            dgu_out(j).start()

            @pl.when(j == chunks - 2)
            def _():
                for i in range(chunks):
                    flat_in(i).start()

        when(j == 0, late[0].wait)
        td[slot] = dot(dytv[...], act[...]).T.astype(BF16)
        when(j == 0, late[1].wait)
        if deep:
            both = dot(atv[...], dgu[...]).astype(BF16)
            tg[slot, 0] = both[:, :hidden]
            tg[slot, 1] = both[:, hidden:]
        else:
            tg[slot, 0] = dot(atv[...], dgu[:, :hidden]).astype(BF16)
            tg[slot, 1] = dot(atv[...], dgu[:, hidden:]).astype(BF16)
        for matrix in (2, 0, 1):
            when(j >= 1, pass_on, j - 1, matrix)
        for matrix in (2, 0, 1):
            send_terms(j, matrix)
        for matrix in (2, 0, 1):
            when(j >= 2, settle, j - 2, matrix)
        return 0

    lax.fori_loop(0, chunks, chunk, 0)
    last = chunks - 1
    if deep:
        for j in range(chunks):
            flat_in(j).wait()
        dgu_out(last).wait()
        tile = wide.shape[1]
        tiles = tokens // tile

        def ins(t):
            s = lax.rem(t, 2)
            return (
                pltpu.make_async_copy(dgu_o.at[rows(t, tile)], wide.at[s], psem.at[s, 0]),
                pltpu.make_async_copy(extra.at[rows(t, tile)], hst.at[s], psem.at[s, 1]),
            )

        def outs(t):
            s = lax.rem(t, 2)
            return (
                pltpu.make_async_copy(dyv.at[rows(t, tile)], dx_o.at[rows(t, tile)], osem.at[s, 0]),
                pltpu.make_async_copy(xtst.at[s], dxt_o.at[:, rows(t, tile)], osem.at[s, 1]),
            )

        for c in ins(0):
            c.start()

        def part(t, _):
            s = lax.rem(t, 2)
            for c in ins(t):
                c.wait()

            @pl.when(t + 1 < tiles)
            def _():
                for c in ins(t + 1):
                    c.start()

            @pl.when(t >= 2)
            def _():
                for c in outs(t):
                    c.wait()

            da = dot(wide[s], flat[...], 1, 1).astype(BF16).astype(F32)
            h = hst[s].astype(F32)
            scale = lax.rsqrt(jnp.mean(h * h, -1, keepdims=True) + 1e-6)
            along = jnp.sum(da * h, -1, keepdims=True) * (scale * scale * scale * (1.0 / dim))
            dh = (da * scale - h * along).astype(BF16)
            dx = (dyv[rows(t, tile), :].astype(F32) + dh.astype(F32)).astype(BF16)
            dyv[rows(t, tile), :] = dx
            xtst[s] = dx.T
            for c in outs(t):
                c.start()

            @pl.when(t == tiles // 4)
            def _():
                for matrix in (2, 0, 1):
                    settle(last - 1, matrix)

            @pl.when(t == tiles // 2)
            def _():
                for matrix in (2, 0, 1):
                    pass_on(last, matrix)

            return 0

        lax.fori_loop(0, tiles, part, 0)
        for t in (tiles - 2, tiles - 1):
            for c in outs(t):
                c.wait()
    else:
        pass_on(last, 2)
        pass_on(last, 0)
        for matrix in (2, 0, 1):
            settle(last - 1, matrix)
        pass_on(last, 1)
    for matrix in (2, 0, 1):
        settle(last, matrix)

    total = sum(sqg[:, i * 128 : (i + 1) * 128] for i in range(sqg.shape[1] // 128))
    total += sum(sqd[:, i * 128 : (i + 1) * 128] for i in range(sqd.shape[1] // 128))
    if deep:
        sq[...] = total
    else:
        tot[me] = total + extra[...]
        peers = (left, right, across)

        def share_out(k):
            return remote(tot.at[me], tot.at[me], csem.at[0, k], csem.at[1, k], {"dp": peers[k]})

        for k in range(3):
            share_out(k).start()
    if not deep:
        for k in range(3):
            share_out(k).wait_send()
            share_out(k).wait_recv()
        sq[...] = tot[0] + tot[1] + tot[2] + tot[3]


def backward(n, deep, a, at_, dy, dyt, d, extra, *gu):
    tokens, dim = dy.shape
    chunks, hidden = d.shape[1:3]
    own, share = dim // n, hidden // n
    V = pltpu.VMEM
    S = jax.ShapeDtypeStruct
    tile, big = 256, 1024
    out_shape = [S((chunks, own, 2 * hidden), BF16), S((chunks, share, dim), BF16), S((8, 128), F32)]
    out_specs = [IN_VMEM] * 3
    scratch = [
        V((tokens, dim), BF16) if deep else V((tokens // big, big, 2 * hidden), F32),
        V((dim, tokens), BF16), V((tokens, dim), BF16), V((dim, tokens), BF16),
        V((tokens, 2 * hidden), BF16), V((tokens, hidden), BF16), V((2, hidden, dim), BF16),
        V((3, 2, dim, hidden), BF16), V((3, hidden, dim), BF16),
        V((chunks, 6, 2, own // 2, hidden), BF16), V((chunks, 6, share // 2, dim), BF16),
        V((8, hidden), F32), V((8, dim), F32),
        DMA((chunks, 18)), DMA((chunks, 18)), DMA((3, tokens // big)), DMA((2, 2)),
    ]
    if deep:
        out_shape += [S((tokens, chunks * 2 * hidden), BF16), S((tokens, dim), BF16), S((dim, tokens), BF16)]
        out_specs += [ANY] * 3
        scratch += [
            V((2, dim, 2 * hidden), BF16), V((dim, chunks * 2 * hidden), BF16), V((2, tile, chunks * 2 * hidden), BF16), V((2, tile, dim), BF16),
            V((2, dim, tile), BF16), DMA((1,)), DMA((chunks,)), DMA((2, 2)), DMA((2, 2)),
        ]
    else:
        scratch += [V((n, 8, 128), F32), DMA((2, 3))]
    return pl.pallas_call(
        functools.partial(backward_kernel, n, deep),
        out_shape=out_shape,
        in_specs=[ANY] * 5 + ([ANY, ANY] if deep else [IN_VMEM]),
        out_specs=out_specs,
        scratch_shapes=scratch,
        compiler_params=pltpu.CompilerParams(collective_id=1 if deep else 2, has_side_effects=True, vmem_limit_bytes=63 * MIB),
        name="backward_deep" if deep else "backward_first",
    )(a, at_, dy, dyt, d, extra, *gu)


def update_kernel(n, count, sq, g0, g1, d0, d1, wg, wu, wd, mg, mu, md, vg, vu, vd, *outs):
    factor = jnp.minimum(1.0, 0.5 * lax.rsqrt(jnp.sum(sq[...], keepdims=True) / count + 1e-30))
    first = pl.program_id(0) == 0
    gu = jnp.where(first, g0[...], g1[...]).astype(F32)
    chunks, hidden = gu.shape[0], gu.shape[2] // 2
    share = hidden // n

    def ordered(start):
        return jnp.concatenate([gu[j, :, start + o * share : start + (o + 1) * share] for o in range(n) for j in range(chunks)], -1)

    grads = (ordered(0), ordered(hidden), jnp.where(first, d0[...], d1[...]).astype(F32))
    for i, (g, w, m, v) in enumerate(zip(grads, (wg, wu, wd), (mg, mu, md), (vg, vu, vd), strict=True)):
        g = g * factor
        new_m = 0.9 * m[0] + 0.1 * g
        new_v = 0.95 * v[0] + 0.05 * g * g
        step = new_m * lax.rsqrt(new_v + 1e-8) + 0.1 * w[0].astype(F32)
        outs[i][0] = (w[0].astype(F32) - 0.02 * step).astype(BF16)
        outs[3 + i][0] = new_m
        outs[6 + i][0] = new_v


def update(n, sq, g0, g1, d0, d1, weights, m, v):
    layers, own, units = weights[0].shape
    down, dim = weights[2].shape[1:]
    chunks = g0.shape[0]
    cut = 4
    count = float(n * sum(w.size for w in weights))
    up = pl.BlockSpec((1, own // cut, units), lambda i, k: (i, k, 0))
    dn = pl.BlockSpec((1, down // cut, dim), lambda i, k: (i, k, 0))
    gs = lambda which: pl.BlockSpec((chunks, own // cut, g0.shape[2]), lambda i, k: (0, jnp.where(i == which, k, (cut - 1) * (1 - which)), 0))
    ds = lambda which: pl.BlockSpec((down // cut, dim), lambda i, k: (jnp.where(i == which, k, (cut - 1) * (1 - which)), 0))
    three = [up, up, dn]
    return pl.pallas_call(
        functools.partial(update_kernel, n, count),
        grid=(layers, cut),
        out_shape=[jax.ShapeDtypeStruct(w.shape, t) for t in (BF16, F32, F32) for w in weights],
        in_specs=[pl.BlockSpec((8, 128), lambda i, k: (0, 0)), gs(0), gs(1), ds(0), ds(1)] + three * 3,
        out_specs=three * 3,
        compiler_params=pltpu.CompilerParams(vmem_limit_bytes=60 * MIB),
        name="update",
    )(sq, g0, g1, d0.reshape(down, dim), d1.reshape(down, dim), *weights, *m, *v)


def solution(mesh):
    n = mesh.shape["dp"]

    def step(x, dy, *arrays):
        weights, m, v = (arrays[i : i + 3] for i in (0, 3, 6))
        gu, d, kept, a0t, dyt, h1, a1, a1t = forward(n, x[0], dy[0], *weights)
        g1, d1, sq1, _, dx, dxt = backward(n, True, a1, a1t, dy[0], dyt, d, h1, gu)
        g0, d0, sq = backward(n, False, kept, a0t, dx, dxt, d, sq1)
        return tuple(update(n, sq, g0, g1, d0, d1, weights, m, v))

    states, cut = P(("rep", "dp"), None, None), P(None, "dp", None)
    return jax.shard_map(
        step,
        mesh=mesh,
        in_specs=(states, states) + (cut,) * 9,
        out_specs=(P("rep", "dp", None),) * 9,
        check_vma=False,
    )
```

```python
import functools

import jax
import jax.numpy as jnp
from jax import lax
from jax.experimental import pallas as pl
from jax.experimental.pallas import tpu as pltpu
from jax.sharding import PartitionSpec as P

MESH = pl.DeviceIdType.MESH
F32, BF16 = jnp.float32, jnp.bfloat16
ANY = pl.BlockSpec(memory_space=pl.ANY)
IN_VMEM = pl.BlockSpec(memory_space=pltpu.VMEM)
DMA = pltpu.SemaphoreType.DMA
MIB = 2**20
WIDTH = 64


def dot(a, b, ca=1, cb=0):
    return lax.dot_general(a, b, (((ca,), (cb,)), ((), ())), preferred_element_type=F32)


def rows(index, size):
    return pl.ds(pl.multiple_of(index * size, size), size)


def at(start, size):
    return pl.ds(pl.multiple_of(start, 16), size)


def normed(h):
    wide = h.astype(F32)
    scale = lax.rsqrt(jnp.mean(wide * wide, -1, keepdims=True) + 1e-6)
    return (wide * scale).astype(BF16)


def around(n):
    me = lax.axis_index("dp")
    return me, lax.rem(me + n - 1, n), lax.rem(me + 1, n), lax.rem(me + 2, n)


def greet(where):
    for device in where:
        pl.semaphore_signal(pltpu.get_barrier_semaphore(), inc=1, device_id=device, device_id_type=MESH)


def meet(where):
    pl.semaphore_wait(pltpu.get_barrier_semaphore(), len(where))


def remote(source, target, send, receive, device):
    return pltpu.make_async_remote_copy(
        src_ref=source, dst_ref=target, send_sem=send, recv_sem=receive, device_id=device, device_id_type=MESH
    )


KINDS = 18


def forward_kernel(
    n, x_h, dy_h, wg, wu, wd, gu_o, d_o, kept_o, at_o, dyt_o, h_o, a1_o, a1t_o,
    xv, av, dyv, acts, gw, dw, gst, tst, tst2, hst, ast, ssem, rsem, xsem, dysem, osem, wsem, ksem,
):
    layers, chunks = gw.shape[0], gw.shape[1]
    tokens, dim = xv.shape
    own, hidden = wg.shape[1], dw.shape[2]
    share, piece = wd.shape[1] // chunks, own // 4
    steps = layers * chunks
    tile = dyv.shape[1]
    tiles = tokens // tile
    me, left, right, across = around(n)
    rep = lax.axis_index("rep")
    core, side = lax.rem(rep, 2), lax.rem(rep // 2, 2)
    mate, twin = rep + 1 - 2 * core, rep + 2 - 4 * side

    friends = [{"dp": left}, {"dp": right}, {"rep": mate}, {"rep": twin}]
    greet(friends)

    def x_in(t):
        return pltpu.make_async_copy(x_h.at[rows(t, tile)], xv.at[rows(t, tile)], xsem.at[t])

    def dy_in(t):
        return pltpu.make_async_copy(dy_h.at[rows(t, tile)], dyv.at[lax.rem(t, 2)], dysem.at[lax.rem(t, 2)])

    def start_x(t, _):
        x_in(t).start()
        return 0

    lax.fori_loop(0, tiles, start_x, 0)
    dy_in(0).start()
    dy_in(1).start()

    def pack(layer):
        gate, up = wg[layer], wu[layer]
        for j in range(chunks):
            pieces = [w[:, o * share * chunks + j * share : o * share * chunks + (j + 1) * share] for w in (gate, up) for o in range(n)]
            start = (layer * chunks + j) * own
            acts[start : start + own, : 2 * hidden] = jnp.concatenate(pieces, -1)

    def place(s, _):
        layer, j = s // chunks, lax.rem(s, chunks)
        gw[layer, j, at(me * own, own), :] = acts[rows(s, own), : 2 * hidden]
        dw[layer, j, at(me * share, share), :] = wd[layer, rows(j, share), :]
        return 0

    pack(0)
    lax.fori_loop(0, chunks, place, 0)
    meet(friends)

    def up_part(s, owner, which):
        return gw.at[s // chunks, lax.rem(s, chunks), at(owner * own + which * 2 * piece + core * piece, piece), :]

    def down_part(s, owner):
        return dw.at[s // chunks, lax.rem(s, chunks), at(owner * share + core * (share // 2), share // 2), :]

    others = (left, right, across)

    def copy(s, kind):
        if kind < 4:
            ref = down_part(s, me) if kind % 2 else up_part(s, me, side)
            device = {"dp": right if kind < 2 else left}
        elif kind == 4:
            ref, device = up_part(s, left, side), {"dp": right}
        elif kind == 5:
            ref, device = down_part(s, right), {"dp": left}
        elif kind < 9:
            ref, device = up_part(s, others[kind - 6], side), {"rep": twin}
        elif kind < 15:
            owner = others[(kind - 9) // 2]
            ref, device = (up_part(s, owner, side) if kind % 2 else down_part(s, owner)), {"rep": mate}
        else:
            ref, device = up_part(s, others[kind - 15], 1 - side), {"rep": mate}
        return remote(ref, ref, ssem.at[s, kind], rsem.at[s, kind], device)

    def weights_out(s):
        layer, j = s // chunks, lax.rem(s, chunks)
        return (
            pltpu.make_async_copy(gw.at[layer, j], gu_o.at[layer, j], wsem.at[s, 0]),
            pltpu.make_async_copy(dw.at[layer, j], d_o.at[layer, j], wsem.at[s, 1]),
        )

    def stage(s, wait, begin):
        @pl.when(s < steps)
        def _():
            for kind in wait:
                copy(s, kind).wait_recv()
            for kind in begin:
                copy(s, kind).start()

    first = ((), (0, 1, 2, 3))
    second = ((0, 1, 2, 3), (4, 5, 6, 7, 9, 10, 11, 12))
    third = ((4, 5), (8, 13, 14))
    fourth = ((6, 7, 8), (15, 16, 17))

    def arrived(s):
        stage(s, range(9, KINDS), ())

        @pl.when(s < steps)
        def _():
            for c in weights_out(s):
                c.start()

    def half_way(j):
        stage(j + 1, *fourth)
        stage(j + 4, *second)
        stage(j + 6, *first)

    def at_end(j):
        stage(j + 3, *third)
        arrived(j + 1)

    def at_out(t, slot):
        return pltpu.make_async_copy(tst.at[slot], at_o.at[:, rows(t, tile)], osem.at[slot, 0])

    def dyt_out(t, slot):
        return pltpu.make_async_copy(tst2.at[slot], dyt_o.at[:, rows(t, tile)], osem.at[slot, 1])

    def prepare(t, slot):
        x_in(t).wait()
        dy_in(t).wait()

        if t >= 2:
            at_out(t, slot).wait()
            dyt_out(t, slot).wait()

        a = normed(xv[rows(t, tile), :])
        av[rows(t, tile), :] = a
        tst[slot] = a.T
        tst2[slot] = dyv[slot].T
        at_out(t, slot).start()
        dyt_out(t, slot).start()

        if t + 2 < tiles:
            dy_in(t + 2).start()

    stage(0, *first)
    stage(1, *first)
    pack(1)
    lax.fori_loop(chunks, steps, place, 0)
    prepare(0, 0)
    prepare(1, 1)
    order = ((0, second), (2, first), 2, (1, second), (3, first), 3, (0, third), 4, (2, second), (4, first), 5, (1, third), 6, (0, fourth), 7)
    for item in order + ((3, second), (5, first), (2, third)):
        if isinstance(item, int):
            prepare(item, item % 2)
        else:
            stage(item[0], *item[1])
    arrived(0)
    big = 2 * tile
    parts = tokens // big

    def keep(j, t):
        slot = lax.rem(t, 2)
        return [
            pltpu.make_async_copy(gst.at[slot, rows(i, tile)], kept_o.at[j, rows(2 * t + i, tile)], ksem.at[slot, i]) for i in range(2)
        ]

    def chunk(j, _):
        def part(t, _):
            @pl.when((j > 0) | (t >= 2))
            def _():
                for c in keep(j, t):
                    c.wait()

            slot = lax.rem(t, 2)
            gu = dot(av[rows(t, big), :], gw[0, j])
            gst[slot] = gu
            for c in keep(j, t):
                c.start()
            gate, up = gu[:, :hidden], gu[:, hidden:]
            acts[rows(t, big), rows(j, hidden)] = (gate * jax.nn.sigmoid(gate) * up).astype(BF16)
            return 0

        lax.fori_loop(0, parts // 2, part, 0)
        half_way(j)
        lax.fori_loop(parts // 2, parts, part, 0)
        at_end(j)
        return 0

    lax.fori_loop(0, chunks, chunk, 0)
    for slot in range(2):
        at_out(0, slot).wait()
        dyt_out(0, slot).wait()
        for c in keep(chunks - 1, slot):
            c.wait()

    def outs(t):
        slot = lax.rem(t, 2)
        return (
            pltpu.make_async_copy(hst.at[slot], h_o.at[rows(t, tile)], osem.at[slot, 3]),
            pltpu.make_async_copy(ast.at[slot], a1_o.at[rows(t, tile)], osem.at[slot, 4]),
            pltpu.make_async_copy(tst.at[slot], a1t_o.at[:, rows(t, tile)], osem.at[slot, 5]),
        )

    def close(t, _):
        slot = lax.rem(t, 2)

        half_way(chunks + t)

        @pl.when(t >= 2)
        def _():
            for c in outs(t):
                c.wait()

        y = dot(acts[rows(t, tile), :], dw[0].reshape(chunks * hidden, dim)).astype(BF16)
        h = (xv[rows(t, tile), :].astype(F32) + y.astype(F32)).astype(BF16)
        a = normed(h)
        hst[slot] = h
        ast[slot] = a
        tst[slot] = a.T
        for c in outs(t):
            c.start()
        at_end(chunks + t)
        return 0

    lax.fori_loop(0, tiles, close, 0)
    for t in (tiles - 2, tiles - 1):
        for c in outs(t):
            c.wait()

    def finish(s, _):
        for kind in range(KINDS):
            copy(s, kind).wait_send()
        for c in weights_out(s):
            c.wait()
        return 0

    lax.fori_loop(0, steps, finish, 0)


def forward(n, x, dy, wg, wu, wd):
    tokens, dim = x.shape
    layers, own, units = wg.shape
    chunks = wd.shape[1] // WIDTH
    hidden = n * WIDTH
    tile = 512
    V = pltpu.VMEM
    S = jax.ShapeDtypeStruct
    return pl.pallas_call(
        functools.partial(forward_kernel, n),
        out_shape=[
            S((layers, chunks, dim, 2 * hidden), BF16), S((layers, chunks, hidden, dim), BF16),
            S((chunks, tokens, 2 * hidden), F32), S((dim, tokens), BF16), S((dim, tokens), BF16),
            S((tokens, dim), BF16), S((tokens, dim), BF16), S((dim, tokens), BF16),
        ],
        in_specs=[ANY, ANY, IN_VMEM, IN_VMEM, IN_VMEM],
        out_specs=[ANY] * 8,
        scratch_shapes=[
            V((tokens, dim), BF16), V((tokens, dim), BF16), V((2, tile, dim), BF16), V((tokens, units), BF16),
            V((layers, chunks, dim, 2 * hidden), BF16), V((layers, chunks, hidden, dim), BF16),
            V((2, 2 * tile, 2 * hidden), F32), V((2, dim, tile), BF16), V((2, dim, tile), BF16), V((2, tile, dim), BF16), V((2, tile, dim), BF16),
            DMA((layers * chunks, KINDS)), DMA((layers * chunks, KINDS)),
            DMA((tokens // tile,)), DMA((2,)), DMA((2, 6)), DMA((layers * chunks, 2)), DMA((2, 2)),
        ],
        compiler_params=pltpu.CompilerParams(collective_id=0, has_side_effects=True, vmem_limit_bytes=63 * MIB),
        name="forward",
    )(x, dy, wg, wu, wd)


def backward_kernel(n, deep, *refs):
    it = iter(refs)
    take = lambda count: [next(it) for _ in range(count)]
    a_h, at_h, dy_h, dyt_h, d_all, extra = take(6)
    d_h = d_all.at[1 if deep else 0]
    if deep:
        gu_h = next(it).at[1]
    og, od, sq = take(3)
    if deep:
        dgu_o, dx_o, dxt_o = take(3)
    av, atv, dyv, dytv, dgu, act, dw, tg, td, rg, rd, sqg, sqd, ssem, rsem, isem, wsem = take(17)
    if deep:
        gw, flat, wide, hst, xtst, dsem, fsem, psem, osem = take(9)
    else:
        tot, csem = take(2)
    tokens, dim = dyv.shape
    chunks, hidden = d_all.shape[1:3]
    own, share = dim // n, hidden // n
    g2, d2 = own // 2, share // 2
    big = 1024
    parts = tokens // big
    me, left, right, across = around(n)

    def a_in(t):
        return pltpu.make_async_copy(a_h.at[rows(t, big)], av.at[rows(t, big)], isem.at[0, t])

    def kept_in(j, t):
        return pltpu.make_async_copy(a_h.at[j, rows(t, big)], av.at[t], isem.at[0, t])

    def dy_in(t):
        return pltpu.make_async_copy(dy_h.at[rows(t, big)], dyv.at[rows(t, big)], isem.at[1, t])

    def late(which):
        source, target = ((dyt_h, dytv), (at_h, atv))[which]
        return [
            pltpu.make_async_copy(source.at[i * own : (i + 1) * own], target.at[i * own : (i + 1) * own], isem.at[2 + which, i])
            for i in range(n)
        ]


    def w_in(j):
        s = lax.rem(j, 2)
        copies = [pltpu.make_async_copy(d_h.at[j], dw.at[s], wsem.at[s, 1])]
        if deep:
            copies.append(pltpu.make_async_copy(gu_h.at[j], gw.at[s], wsem.at[s, 0]))
        return copies

    friends = [{"dp": left}, {"dp": right}] + ([] if deep else [{"dp": across}])
    greet(friends)
    for c in w_in(0):
        c.start()
    if not deep:
        for t in range(parts):
            kept_in(0, t).start()
    for t in range(parts):
        dy_in(t).start()
        if deep:
            a_in(t).start()
    sqg[...] = jnp.zeros_like(sqg)
    sqd[...] = jnp.zeros_like(sqd)
    meet(friends)

    def spot(j, matrix, owner, which):
        if matrix < 2:
            return tg, (lax.rem(j, 3), matrix, at(owner * own + which * g2, g2))
        return td, (lax.rem(j, 3), at(owner * share + which * d2, d2))

    def landing(j, unit, matrix):
        return (rg, (j, unit, matrix)) if matrix < 2 else (rd, (j, unit))

    def copy(j, unit, matrix):
        owner, which = ((across, 0), (across, 1), (right, 1), (left, 0), (right, 0), (left, 1))[unit]
        source, place = spot(j, matrix, owner, which)
        target, index = landing(j, unit, matrix)
        sem = 3 * unit + matrix
        return remote(source.at[place], target.at[index], ssem.at[j, sem], rsem.at[j, sem], {"dp": right if unit % 2 == 0 else left})

    def send_terms(j, matrix):
        for unit in (0, 1, 2, 3):
            copy(j, unit, matrix).start()

    def pass_on(j, matrix):
        for unit, owner, which in ((0, right, 0), (1, left, 1)):
            copy(j, unit, matrix).wait_recv()
            term, place = spot(j, matrix, owner, which)
            got, index = landing(j, unit, matrix)
            term[place] = (term[place].astype(F32) + got[index].astype(F32)).astype(BF16)
            copy(j, unit + 4, matrix).start()

    def settle(j, matrix):
        for unit in (2, 3, 4, 5):
            copy(j, unit, matrix).wait_recv()
        for which, single, summed in ((0, 3, 4), (1, 2, 5)):
            term, place = spot(j, matrix, me, which)
            got, one = landing(j, single, matrix)
            _, other = landing(j, summed, matrix)
            g = (term[place].astype(F32) + got[one].astype(F32) + got[other].astype(F32)).astype(BF16)
            if matrix < 2:
                og[j, which * g2 : (which + 1) * g2, matrix * hidden : (matrix + 1) * hidden] = g
            else:
                od[j, which * d2 : (which + 1) * d2, :] = g
            g = g.astype(F32)
            total = sqg if matrix < 2 else sqd
            total[...] += jnp.sum((g * g).reshape(g.shape[0] // 8, 8, g.shape[1]), axis=0)
        for unit in range(6):
            copy(j, unit, matrix).wait_send()

    def when(condition, what, *args):
        @pl.when(condition)
        def _():
            what(*args)

    if deep:
        dgu_out = lambda j: pltpu.make_async_copy(dgu, dgu_o.at[:, rows(j, 2 * hidden)], dsem.at[0])
        flat_in = lambda j: pltpu.make_async_copy(gu_h.at[j], flat.at[:, j * 2 * hidden : (j + 1) * 2 * hidden], fsem.at[j])

    def chunk(j, _):
        s, slot = lax.rem(j, 2), lax.rem(j, 3)
        for c in w_in(j):
            c.wait()

        @pl.when(j + 1 < chunks)
        def _():
            for c in w_in(j + 1):
                c.start()

        if deep:

            @pl.when(j >= 1)
            def _():
                dgu_out(j - 1).wait()

        def part(t, _):
            @pl.when(j == 0)
            def _():
                dy_in(t).wait()
                if deep:
                    a_in(t).wait()

                @pl.when(t < 2)
                def _():
                    for which in range(2):

                        @pl.when(t == which)
                        def _():
                            for c in late(which):
                                c.start()


            r = rows(t, big)
            if deep:
                gu = dot(av[r, :], gw[s])
            else:
                kept_in(j, t).wait()
                gu = av[t]
            dact = dot(dyv[r, :], dw[s], 1, 1).astype(BF16).astype(F32)
            gate, up = gu[:, :hidden], gu[:, hidden:]
            sig = jax.nn.sigmoid(gate)
            silu = gate * sig
            act[r, :] = (silu * up).astype(BF16)
            dgu[r, hidden:] = (dact * silu).astype(BF16)
            dgu[r, :hidden] = (dact * up * (sig + silu * (1 - sig))).astype(BF16)
            if not deep:
                when(j + 1 < chunks, lambda: kept_in(j + 1, t).start())
            return 0

        lax.fori_loop(0, parts, part, 0)
        if deep:
            dgu_out(j).start()

            @pl.when(j == chunks - 2)
            def _():
                for i in range(chunks):
                    flat_in(i).start()

        when(j == 0, lambda: [c.wait() for c in late(0)])
        td[slot] = dot(dytv[...], act[...]).T.astype(BF16)
        when(j == 0, lambda: [c.wait() for c in late(1)])
        if deep:
            both = dot(atv[...], dgu[...]).astype(BF16)
            tg[slot, 0] = both[:, :hidden]
            tg[slot, 1] = both[:, hidden:]
        else:
            tg[slot, 0] = dot(atv[...], dgu[:, :hidden]).astype(BF16)
            tg[slot, 1] = dot(atv[...], dgu[:, hidden:]).astype(BF16)
        for matrix in (2, 0, 1):
            when(j >= 1, pass_on, j - 1, matrix)
        for matrix in (2, 0, 1):
            send_terms(j, matrix)
        for matrix in (2, 0, 1):
            when(j >= 2, settle, j - 2, matrix)
        return 0

    lax.fori_loop(0, chunks, chunk, 0)
    last = chunks - 1
    if deep:
        for j in range(chunks):
            flat_in(j).wait()
        dgu_out(last).wait()
        tile = wide.shape[1]
        tiles = tokens // tile

        def ins(t):
            s = lax.rem(t, 2)
            return (
                *(
                    pltpu.make_async_copy(dgu_o.at[rows(4 * t + i, tile // 4)], wide.at[s, rows(i, tile // 4)], psem.at[s, i])
                    for i in range(4)
                ),
                pltpu.make_async_copy(extra.at[rows(t, tile)], hst.at[s], psem.at[s, 4]),
            )

        def outs(t):
            s = lax.rem(t, 2)
            return (
                pltpu.make_async_copy(dyv.at[rows(t, tile)], dx_o.at[rows(t, tile)], osem.at[s, 0]),
                pltpu.make_async_copy(xtst.at[s], dxt_o.at[:, rows(t, tile)], osem.at[s, 1]),
            )

        for c in ins(0):
            c.start()

        def part(t, _):
            s = lax.rem(t, 2)
            for c in ins(t):
                c.wait()

            @pl.when(t + 1 < tiles)
            def _():
                for c in ins(t + 1):
                    c.start()

            @pl.when(t >= 2)
            def _():
                for c in outs(t):
                    c.wait()

            da = dot(wide[s], flat[...], 1, 1).astype(BF16).astype(F32)
            h = hst[s].astype(F32)
            scale = lax.rsqrt(jnp.mean(h * h, -1, keepdims=True) + 1e-6)
            along = jnp.sum(da * h, -1, keepdims=True) * (scale * scale * scale * (1.0 / dim))
            dh = (da * scale - h * along).astype(BF16)
            dx = (dyv[rows(t, tile), :].astype(F32) + dh.astype(F32)).astype(BF16)
            dyv[rows(t, tile), :] = dx
            xtst[s] = dx.T
            for c in outs(t):
                c.start()

            @pl.when(t == tiles // 4)
            def _():
                for matrix in (2, 0, 1):
                    settle(last - 1, matrix)

            @pl.when(t == tiles // 2)
            def _():
                for matrix in (2, 0, 1):
                    pass_on(last, matrix)

            return 0

        lax.fori_loop(0, tiles, part, 0)
        for t in (tiles - 2, tiles - 1):
            for c in outs(t):
                c.wait()
    else:
        pass_on(last, 2)
        pass_on(last, 0)
        for matrix in (2, 0, 1):
            settle(last - 1, matrix)
        pass_on(last, 1)
    for matrix in (2, 0, 1):
        settle(last, matrix)

    total = sum(sqg[:, i * 128 : (i + 1) * 128] for i in range(sqg.shape[1] // 128))
    total += sum(sqd[:, i * 128 : (i + 1) * 128] for i in range(sqd.shape[1] // 128))
    if deep:
        sq[...] = total
    else:
        tot[me] = total + extra[...]
        peers = (left, right, across)

        def share_out(k):
            return remote(tot.at[me], tot.at[me], csem.at[0, k], csem.at[1, k], {"dp": peers[k]})

        for k in range(3):
            share_out(k).start()
    if not deep:
        for k in range(3):
            share_out(k).wait_send()
            share_out(k).wait_recv()
        sq[...] = tot[0] + tot[1] + tot[2] + tot[3]


def backward(n, deep, a, at_, dy, dyt, d, extra, *gu):
    tokens, dim = dy.shape
    chunks, hidden = d.shape[1:3]
    own, share = dim // n, hidden // n
    V = pltpu.VMEM
    S = jax.ShapeDtypeStruct
    tile, big = 256, 1024
    out_shape = [S((chunks, own, 2 * hidden), BF16), S((chunks, share, dim), BF16), S((8, 128), F32)]
    out_specs = [IN_VMEM] * 3
    scratch = [
        V((tokens, dim), BF16) if deep else V((tokens // big, big, 2 * hidden), F32),
        V((dim, tokens), BF16), V((tokens, dim), BF16), V((dim, tokens), BF16),
        V((tokens, 2 * hidden), BF16), V((tokens, hidden), BF16), V((2, hidden, dim), BF16),
        V((3, 2, dim, hidden), BF16), V((3, hidden, dim), BF16),
        V((chunks, 6, 2, own // 2, hidden), BF16), V((chunks, 6, share // 2, dim), BF16),
        V((8, hidden), F32), V((8, dim), F32),
        DMA((chunks, 18)), DMA((chunks, 18)), DMA((4, max(n, tokens // big))), DMA((2, 2)),
    ]
    if deep:
        out_shape += [S((tokens, chunks * 2 * hidden), BF16), S((tokens, dim), BF16), S((dim, tokens), BF16)]
        out_specs += [ANY] * 3
        scratch += [
            V((2, dim, 2 * hidden), BF16), V((dim, chunks * 2 * hidden), BF16), V((2, tile, chunks * 2 * hidden), BF16), V((2, tile, dim), BF16),
            V((2, dim, tile), BF16), DMA((1,)), DMA((chunks,)), DMA((2, 5)), DMA((2, 2)),
        ]
    else:
        scratch += [V((n, 8, 128), F32), DMA((2, 3))]
    return pl.pallas_call(
        functools.partial(backward_kernel, n, deep),
        out_shape=out_shape,
        in_specs=[ANY] * 5 + ([ANY, ANY] if deep else [IN_VMEM]),
        out_specs=out_specs,
        scratch_shapes=scratch,
        compiler_params=pltpu.CompilerParams(collective_id=1 if deep else 2, has_side_effects=True, vmem_limit_bytes=63 * MIB),
        name="backward_deep" if deep else "backward_first",
    )(a, at_, dy, dyt, d, extra, *gu)


def update_kernel(n, count, sq, g0, g1, d0, d1, wg, wu, wd, mg, mu, md, vg, vu, vd, *outs):
    factor = jnp.minimum(1.0, 0.5 * lax.rsqrt(jnp.sum(sq[...], keepdims=True) / count + 1e-30))
    first = pl.program_id(0) == 0
    gu = jnp.where(first, g0[...], g1[...]).astype(F32)
    chunks, hidden = gu.shape[0], gu.shape[2] // 2
    share = hidden // n

    def ordered(start):
        return jnp.concatenate([gu[j, :, start + o * share : start + (o + 1) * share] for o in range(n) for j in range(chunks)], -1)

    grads = (ordered(0), ordered(hidden), jnp.where(first, d0[...], d1[...]).astype(F32))
    for i, (g, w, m, v) in enumerate(zip(grads, (wg, wu, wd), (mg, mu, md), (vg, vu, vd), strict=True)):
        g = g * factor
        new_m = 0.9 * m[0] + 0.1 * g
        new_v = 0.95 * v[0] + 0.05 * g * g
        step = new_m * lax.rsqrt(new_v + 1e-8) + 0.1 * w[0].astype(F32)
        outs[i][0] = (w[0].astype(F32) - 0.02 * step).astype(BF16)
        outs[3 + i][0] = new_m
        outs[6 + i][0] = new_v


def update(n, sq, g0, g1, d0, d1, weights, m, v):
    layers, own, units = weights[0].shape
    down, dim = weights[2].shape[1:]
    chunks = g0.shape[0]
    cut = 4
    count = float(n * sum(w.size for w in weights))
    up = pl.BlockSpec((1, own // cut, units), lambda i, k: (i, k, 0))
    dn = pl.BlockSpec((1, down // cut, dim), lambda i, k: (i, k, 0))
    gs = lambda which: pl.BlockSpec((chunks, own // cut, g0.shape[2]), lambda i, k: (0, jnp.where(i == which, k, (cut - 1) * (1 - which)), 0))
    ds = lambda which: pl.BlockSpec((down // cut, dim), lambda i, k: (jnp.where(i == which, k, (cut - 1) * (1 - which)), 0))
    three = [up, up, dn]
    return pl.pallas_call(
        functools.partial(update_kernel, n, count),
        grid=(layers, cut),
        out_shape=[jax.ShapeDtypeStruct(w.shape, t) for t in (BF16, F32, F32) for w in weights],
        in_specs=[pl.BlockSpec((8, 128), lambda i, k: (0, 0)), gs(0), gs(1), ds(0), ds(1)] + three * 3,
        out_specs=three * 3,
        compiler_params=pltpu.CompilerParams(vmem_limit_bytes=60 * MIB),
        name="update",
    )(sq, g0, g1, d0.reshape(down, dim), d1.reshape(down, dim), *weights, *m, *v)


def solution(mesh):
    n = mesh.shape["dp"]

    def step(x, dy, *arrays):
        weights, m, v = (arrays[i : i + 3] for i in (0, 3, 6))
        gu, d, kept, a0t, dyt, h1, a1, a1t = forward(n, x[0], dy[0], *weights)
        g1, d1, sq1, _, dx, dxt = backward(n, True, a1, a1t, dy[0], dyt, d, h1, gu)
        g0, d0, sq = backward(n, False, kept, a0t, dx, dxt, d, sq1)
        return tuple(update(n, sq, g0, g1, d0, d1, weights, m, v))

    states, cut = P(("rep", "dp"), None, None), P(None, "dp", None)
    return jax.shard_map(
        step,
        mesh=mesh,
        in_specs=(states, states) + (cut,) * 9,
        out_specs=(P("rep", "dp", None),) * 9,
        check_vma=False,
    )
```
